32 devices in a mesh: row: 2 (over y), col: 4 (over x, core), band: 4 (over z).
Axes of the slice: x: 2, y: 2, z: 4, core: 2. Of those that a mesh axis runs over, the one named last changes fastest.
Arguments:
- noisy: float32 [224, 32, 4096], P('band', 'row', 'col'), may hold values from -4 to 4
- weight_map: float32 [32, 4096], P('row', 'col'), may hold values from 1.5 to 12
Outputs:
- denoised: float32 [224, 32, 4096], P('band', 'row', 'col')
The draws below stay inside these ranges and needn't reach their ends.
All inputs are finite; a program needn't handle non-finite values.
Results may differ from the reference program's by a relative error of at most 0.0001.
Values sent between devices are 32-bit elements; how exact they have to be, the bound alone decides.
A program may use at most 64 MiB of HBM per device.

```python
import math
import jax
import jax.numpy as jnp
from jax import lax

BANDS = 224
COLS = 4096
ITERS = 4
ROWS = 32


def draw_noisy(key, part):
    key_center, key_texture = jax.random.split(jax.random.fold_in(key, 17))
    center = jax.random.randint(key_center, (), 0, BANDS).astype(jnp.float32)
    spread = BANDS / 16.0
    texture = jnp.clip(jax.random.normal(key_texture, (BANDS, ROWS, COLS), jnp.float32), -4.0, 4.0)
    offset = (jnp.arange(BANDS, dtype=jnp.float32) - center) / spread
    profile = 0.1 + 0.9 * jnp.exp(-0.5 * offset * offset)
    return (profile[:, None, None] * texture).astype(jnp.float32)


def shard_levels(key, extent, cuts, low, top_value):
    level = 1.0
    for dim, shards_of in cuts:
        steps = jax.random.uniform(jax.random.fold_in(jax.random.fold_in(key, 6), dim), (shards_of,), jnp.float32, low / len(cuts), top_value / len(cuts))
        level = level * jnp.repeat(jnp.exp(steps), extent[dim] // shards_of).reshape((-1,) + (1,) * (len(extent) - 1 - dim))
    return level


def setup_inputs(seed: int = 0) -> dict:
    key_of = jax.random.split(jax.random.key(seed), 3)
    noisy = draw_noisy(jax.random.fold_in(key_of[2], 71), 0)
    weight_map = jnp.clip(jnp.exp(math.log(12.0) - 2.0794415 * jax.random.uniform(key_of[1], (ROWS, COLS), jnp.float32) ** shard_levels(key_of[1], (ROWS, COLS), ((0, 2), (1, 4)), -0.2, 0.2)), 1.5, 12.0)
    return {"noisy": noisy, "weight_map": weight_map}


dual_step = 0.35
primal_step = 0.35

def forward_diff(field):
    zeros_row = jnp.zeros_like(field[:, :1, :])
    zeros_col = jnp.zeros_like(field[:, :, :1])
    grad_x = jnp.concatenate([field[:, 1:, :] - field[:, :-1, :], zeros_row], axis=1)
    grad_y = jnp.concatenate([field[:, :, 1:] - field[:, :, :-1], zeros_col], axis=2)
    return (grad_x, grad_y)

def divergence(first, second):
    masked_a = first.at[:, -1, :].set(0.0)
    masked_b = second.at[:, :, -1].set(0.0)
    above = jnp.concatenate([jnp.zeros_like(masked_a[:, :1, :]), masked_a[:, :-1, :]], axis=1)
    left = jnp.concatenate([jnp.zeros_like(masked_b[:, :, :1]), masked_b[:, :, :-1]], axis=2)
    return masked_a - above + (masked_b - left)

def reference(noisy, weight_map):
    groups = math.gcd(BANDS, 8)
    rows = noisy.shape[1]
    cols = noisy.shape[2]
    source = noisy.reshape(groups, BANDS // groups, rows, cols)
    primal = source
    extra = source
    dual_x = jnp.zeros_like(source)
    dual_y = jnp.zeros_like(source)
    for step in range(ITERS):

        def dual_part(items):
            ubar, first, second = items
            grad_x, grad_y = forward_diff(ubar)
            qx = first + dual_step * grad_x
            qy = second + dual_step * grad_y
            return (qx, qy, lax.optimization_barrier(jnp.sum(qx * qx + qy * qy, axis=0)))
        qxs, qys, partial_value = lax.map(dual_part, (extra, dual_x, dual_y))
        squares = lax.optimization_barrier(jnp.sum(partial_value, axis=0))
        scale = weight_map / jnp.maximum(weight_map, jnp.sqrt(1.0 + squares))

        def primal_part(items):
            qx, qy, older, given = items
            first = scale * qx
            second = scale * qy
            newer = (older + primal_step * divergence(first, second) + primal_step * given) / (1.0 + primal_step)
            return (first, second, newer, 2.0 * newer - older)
        dual_x, dual_y, primal, extra = lax.map(primal_part, (qxs, qys, primal, source))
    return primal.reshape(BANDS, rows, cols)
```

```python
import functools

import jax
import jax.numpy as jnp
from jax import lax
from jax.experimental import pallas as pl
from jax.experimental.pallas import tpu as pltpu
from jax.sharding import PartitionSpec as P

ITERS = 4
dual_step = 0.35
primal_step = 0.35
KEEP = 1.0 / (1.0 + primal_step)
GAIN = primal_step / (1.0 + primal_step)
STEP = GAIN * dual_step
LANES = 128
USEFUL = LANES - 2 * ITERS
MESH = pl.DeviceIdType.MESH


def kernel(n_row, n_col, n_band, x_ref, w_ref, out_ref,
           X, WV, N, U, W, QX, QY, HU, HD, E, ER, EL, WT, SC, CY, S, SE, R, RE, RB,
           in_sem, w_sem, ys, yr, xs, xr, zs, zr):
    bands, rows, cols = x_ref.shape
    tiles = N.shape[0]
    groups = bands // 8
    last = rows - 1
    ri = lax.axis_index("row")
    ci = lax.axis_index("col")
    bi = lax.axis_index("band")
    has_up = ri > 0
    has_down = ri < n_row - 1
    has_left = ci > 0
    has_right = ci < n_col - 1
    full = pl.ds(0, bands)

    fetches = [pltpu.make_async_copy(x_ref.at[:, r, :], X.at[r, 0:bands, LANES:LANES + cols], in_sem.at[r])
               for r in range(rows)]
    for copy in fetches:
        copy.start()
    fetch_w = pltpu.make_async_copy(w_ref, WV, w_sem.at[0])
    fetch_w.start()

    barrier = pltpu.get_barrier_semaphore()
    for cond, axis, target in ((has_up, "row", ri - 1), (has_down, "row", ri + 1),
                               (has_left, "col", ci - 1), (has_right, "col", ci + 1)):
        @pl.when(cond)
        def _():
            pl.semaphore_signal(barrier, inc=1, device_id={axis: target}, device_id_type=MESH)
    for d in range(1, n_band):
        pl.semaphore_signal(barrier, inc=1, device_id={"band": lax.rem(bi + d, n_band)}, device_id_type=MESH)
    count = (n_band - 1 + has_up.astype(jnp.int32) + has_down.astype(jnp.int32)
             + has_left.astype(jnp.int32) + has_right.astype(jnp.int32))

    def y_pair(k, j):
        span = pl.ds(0, N.shape[2]) if k == 0 else full
        src = N if k == 0 else W
        up = pltpu.make_async_remote_copy(
            src_ref=src.at[j, 0], dst_ref=HU.at[k, j, span], send_sem=ys.at[0, k, j], recv_sem=yr.at[0, k, j],
            device_id={"row": ri - 1}, device_id_type=MESH)
        down = pltpu.make_async_remote_copy(
            src_ref=src.at[j, last], dst_ref=HD.at[k, j, span], send_sem=ys.at[1, k, j], recv_sem=yr.at[1, k, j],
            device_id={"row": ri + 1}, device_id_type=MESH)
        return up, down

    def y_start(k, j):
        up, down = y_pair(k, j)

        @pl.when(has_up)
        def _():
            up.start()

        @pl.when(has_down)
        def _():
            down.start()

    def y_recv(k, j):
        up, down = y_pair(k, j)

        @pl.when(has_down)
        def _():
            up.wait_recv()

        @pl.when(has_up)
        def _():
            down.wait_recv()

    def y_sent(k, j):
        up, down = y_pair(k, j)

        @pl.when(has_up)
        def _():
            up.wait_send()

        @pl.when(has_down)
        def _():
            down.wait_send()

    def z_copy(k, j, d, part):
        src, dst = ((S, R), (SE, RE))[part]
        return pltpu.make_async_remote_copy(
            src_ref=src.at[k, j], dst_ref=dst.at[k, j, d - 1],
            send_sem=zs.at[k, j, d - 1, part], recv_sem=zr.at[k, j, d - 1, part],
            device_id={"band": lax.rem(bi + d, n_band)}, device_id_type=MESH)

    def z_start(k, j, part):
        for d in range(1, n_band):
            z_copy(k, j, d, part).start()

    def scale_of(weight, squares):
        return jnp.minimum(1.0, weight * lax.rsqrt(1.0 + squares * (1.0 / (GAIN * GAIN))))

    def sync(k, j):
        for part in range(2):
            for d in range(1, n_band):
                z_copy(k, j, d, part).wait_recv()
        acc = S[k, j]
        edge = SE[k, j]
        for d in range(1, n_band):
            acc = acc + R[k, j, d - 1]
            edge = edge + RE[k, j, d - 1]
        SC[j, 0:rows] = scale_of(WT[j, 0:rows], acc)
        SC[j, last:last + 2] = scale_of(WT[j, last:last + 2], edge)

    def to_right(v):
        return pltpu.roll(v, 1, 1)

    def to_left(v):
        return pltpu.roll(v, LANES - 1, 1)

    def squares(qx, qy):
        return jnp.sum(qx * qx + qy * qy, axis=0, keepdims=True)

    def order(i):
        return lax.rem(i + 1, tiles)

    lane = lax.broadcasted_iota(jnp.int32, (8, LANES), 1)
    for j in range(tiles):
        column = ci * cols + j * USEFUL - ITERS + lane
        CY[j] = jnp.where((column >= 0) & (column < n_col * cols - 1), STEP, 0.0)
    S[:, :, last:rows, :] = jnp.zeros((ITERS, tiles, 1, LANES), jnp.float32)
    RB[...] = jnp.zeros_like(RB)

    @pl.when(jnp.logical_not(has_down))
    def _():
        HU[...] = jnp.zeros_like(HU)

    @pl.when(jnp.logical_not(has_up))
    def _():
        HD[...] = jnp.zeros_like(HD)

    @pl.when(jnp.logical_not(has_right))
    def _():
        ER[...] = jnp.zeros_like(ER)

    @pl.when(jnp.logical_not(has_left))
    def _():
        EL[...] = jnp.zeros_like(EL)

    fetch_w.wait()

    def put_weight(r, _):
        X[r, pl.ds(bands, 8), LANES:LANES + cols] = jnp.broadcast_to(WV[pl.ds(r, 1), :], (8, cols))
        return 0
    lax.fori_loop(0, rows, put_weight, 0)

    for copy in fetches:
        copy.wait()

    pitch = 2 * ITERS
    spot = lax.broadcasted_iota(jnp.int32, (8, LANES), 1)

    def pack(g, _):
        span = pl.ds(pl.multiple_of(g * 8, 8), 8)
        acc = jnp.zeros((8, LANES), jnp.float32)
        for r in range(rows):
            at = r * pitch
            head = pltpu.roll(X[r, span, LANES:2 * LANES], at % LANES, 1)
            tail = pltpu.roll(X[r, span, cols:cols + LANES], (at + pitch) % LANES, 1)
            acc = jnp.where((spot >= at) & (spot < at + ITERS), head, acc)
            acc = jnp.where((spot >= at + ITERS) & (spot < at + pitch), tail, acc)
        E[span] = acc
        return 0
    lax.fori_loop(0, groups + 1, pack, 0)

    pl.semaphore_wait(barrier, count)

    e_left = pltpu.make_async_remote_copy(
        src_ref=E, dst_ref=ER, send_sem=xs.at[0], recv_sem=xr.at[0],
        device_id={"col": ci - 1}, device_id_type=MESH)
    e_right = pltpu.make_async_remote_copy(
        src_ref=E, dst_ref=EL, send_sem=xs.at[1], recv_sem=xr.at[1],
        device_id={"col": ci + 1}, device_id_type=MESH)

    @pl.when(has_left)
    def _():
        e_left.start()

    @pl.when(has_right)
    def _():
        e_right.start()

    def begin(j):
        base = j * USEFUL + LANES - ITERS
        at = base // LANES
        turn = base - at * LANES
        lo = pl.ds(pl.multiple_of(at * LANES, LANES), LANES)
        hi = pl.ds(pl.multiple_of(at * LANES + LANES, LANES), LANES)
        near = lax.broadcasted_iota(jnp.int32, (1, LANES), 1) < LANES - turn
        back = lax.rem(LANES - turn, LANES)

        def take(r):
            v = jnp.where(near, pltpu.roll(X[r, :, lo], back, 1), pltpu.roll(X[r, :, hi], back, 1))
            N[j, r] = v
            WT[j, r:r + 1] = v[bands:bands + 1]
            return v[0:bands]

        cy = CY[j, 0:1]
        old = take(0)
        end = take(last)
        y_start(0, j)
        for r in range(1, rows):
            new = take(r) if r < last else end
            qx = STEP * (new - old)
            qy = cy * (to_left(old) - old)
            QX[j, r - 1] = qx
            QY[j, r - 1] = qy
            S[0, j, r - 1:r] = squares(qx, qy)
            old = new
        z_start(0, j, 0)

    def begin_loop(lo, hi):
        def one(i, _):
            begin(order(i))
            return 0
        lax.fori_loop(lo, hi, one, 0)

    inner = sum(1 for j in range(1, tiles) if j * USEFUL + LANES - ITERS <= cols)
    begin_loop(0, inner)

    @pl.when(has_right)
    def _():
        e_left.wait_recv()

    @pl.when(has_left)
    def _():
        e_right.wait_recv()

    def unpack(g, _):
        span = pl.ds(pl.multiple_of(g * 8, 8), 8)
        from_right, from_left = ER[span], EL[span]
        for r in range(rows):
            at = r * pitch
            X[r, span, cols + LANES:cols + 2 * LANES] = pltpu.roll(from_right, (LANES - at) % LANES, 1)
            X[r, span, 0:LANES] = pltpu.roll(from_left, (2 * LANES - at - pitch) % LANES, 1)
        return 0
    lax.fori_loop(0, groups + 1, unpack, 0)
    begin_loop(inner, tiles)

    cx_last = jnp.where(has_down, STEP, 0.0)
    cx_above = jnp.where(has_up, STEP, 0.0)

    def edges(k, j):
        y_recv(k, j)
        field = N if k == 0 else W
        if k == 0:
            WT[j, rows:rows + 1] = HD[0, j, bands:bands + 1]
        cy = CY[j, 0:1]
        end, top = field[j, last, full], field[j, 0, full]
        below, above = HU[k, j, full], HD[k, j, full]
        for i, r, own, nxt, cx in ((0, last, end, below, cx_last), (1, rows, above, top, cx_above)):
            qx = cx * (nxt - own)
            qy = cy * (to_left(own) - own)
            if k > 0:
                sc = SC[j, r:r + 1]
                qx = sc * QX[j, r] + qx
                qy = sc * QY[j, r] + qy
            QX[j, r] = qx
            QY[j, r] = qy
            SE[k, j, i:i + 1] = squares(qx, qy)
        z_start(k, j, 1)

    def edge_loop(k):
        def one(i, _):
            edges(k, order(i))
            return 0
        lax.fori_loop(0, tiles, one, 0)

    edge_loop(0)

    def primal(j, r, px, pu, py, first):
        div = (px - pu) + (py - to_right(py))
        given = N[j, r, full]
        if first:
            return given + div, given
        u = U[j, r]
        return KEEP * u + (GAIN * given + div), u

    def step(k, j):
        first = k == 1
        if k > 1:
            y_sent(k - 1, j)
        sync(k - 1, j)

        def primal_row(r, px, pu, py):
            new, u = primal(j, r, px, pu, py, first)
            U[j, r] = new
            w = 2.0 * new - u
            W[j, r] = w
            return w

        def px_of(r):
            return SC[j, r:r + 1] * QX[j, r]

        def py_of(r):
            return SC[j, r:r + 1] * QY[j, r]

        px, py = px_of(0), py_of(0)
        w = primal_row(0, px, px_of(rows), py)
        end = primal_row(last, px_of(last), px_of(last - 1), py_of(last))
        y_start(k, j)
        cy = CY[j, 0:1]
        for r in range(1, rows):
            if r < last:
                px_new, py_new = px_of(r), py_of(r)
                w_new = primal_row(r, px_new, px, py_new)
            else:
                px_new, py_new, w_new = None, None, end
            qx = px + STEP * (w_new - w)
            qy = py + cy * (to_left(w) - w)
            QX[j, r - 1] = qx
            QY[j, r - 1] = qy
            S[k, j, r - 1:r] = squares(qx, qy)
            px, py, w = px_new, py_new, w_new
        z_start(k, j, 0)

    for k in range(1, ITERS):
        def one(i, _, k=k):
            step(k, order(i))
            return 0
        lax.fori_loop(0, tiles, one, 0)
        edge_loop(k)

    wide_lane = lax.broadcasted_iota(jnp.int32, (1, LANES), 1)

    def finish(j, wrap):
        sync(ITERS - 1, j)
        base = j * USEFUL + LANES - ITERS
        at = base // LANES - 1
        turn = base - (at + 1) * LANES
        if wrap:
            spot, keep = pl.ds(0, LANES), wide_lane >= USEFUL
        else:
            spot, keep = pl.ds(pl.multiple_of(at * LANES, LANES), LANES), wide_lane >= j * USEFUL - at * LANES
        pu = SC[j, rows:rows + 1] * QX[j, rows]
        for r in range(rows):
            sc = SC[j, r:r + 1]
            px = sc * QX[j, r]
            new, _ = primal(j, r, px, pu, sc * QY[j, r], False)
            turned = pltpu.roll(new, turn, 1)
            if wrap:
                out_ref[r, :, spot] = jnp.where(keep, out_ref[r, :, spot], turned)
            else:
                out_ref[r, :, spot] = jnp.where(keep, turned, RB[r])
                RB[r] = turned
            pu = px

    def finish_one(j, _):
        finish(j, False)
        return 0
    lax.fori_loop(1, tiles, finish_one, 0)
    finish(0, True)

    @pl.when(has_left)
    def _():
        e_left.wait_send()

    @pl.when(has_right)
    def _():
        e_right.wait_send()

    def drain(j, _):
        y_sent(0, j)
        y_sent(ITERS - 1, j)
        for k in range(ITERS):
            for d in range(1, n_band):
                for part in range(2):
                    z_copy(k, j, d, part).wait_send()
        return 0
    lax.fori_loop(0, tiles, drain, 0)


def local(n_row, n_col, n_band, noisy, weight_map):
    bands, rows, cols = noisy.shape
    padded = -(-bands // 8) * 8
    x = noisy
    if padded != bands:
        x = jnp.pad(x, ((0, padded - bands), (0, 0), (0, 0)))
    f32 = jnp.float32
    tiles = -(-cols // USEFUL)
    wide = cols + 2 * LANES
    extra = -(-(rows + 1) // 8) * 8
    peers = n_band - 1
    dma = pltpu.SemaphoreType.DMA
    vmem = pltpu.VMEM
    out = pl.pallas_call(
        functools.partial(kernel, n_row, n_col, n_band),
        out_shape=jax.ShapeDtypeStruct((rows, padded, cols), f32),
        in_specs=[pl.BlockSpec(memory_space=pltpu.HBM), pl.BlockSpec(memory_space=pltpu.HBM)],
        out_specs=pl.BlockSpec(memory_space=vmem),
        scratch_shapes=[
            vmem((rows, padded + 8, wide), f32),
            vmem((rows, cols), f32),
            vmem((tiles, rows, padded + 8, LANES), f32),
            vmem((tiles, rows, padded, LANES), f32),
            vmem((tiles, rows, padded, LANES), f32),
            vmem((tiles, rows + 1, padded, LANES), f32),
            vmem((tiles, rows + 1, padded, LANES), f32),
            vmem((ITERS, tiles, padded + 8, LANES), f32),
            vmem((ITERS, tiles, padded + 8, LANES), f32),
            vmem((padded + 8, LANES), f32),
            vmem((padded + 8, LANES), f32),
            vmem((padded + 8, LANES), f32),
            vmem((tiles, extra, LANES), f32),
            vmem((tiles, extra, LANES), f32),
            vmem((tiles, 8, LANES), f32),
            vmem((ITERS, tiles, rows, LANES), f32),
            vmem((ITERS, tiles, 2, LANES), f32),
            vmem((ITERS, tiles, peers, rows, LANES), f32),
            vmem((ITERS, tiles, peers, 2, LANES), f32),
            vmem((rows, padded, LANES), f32),
            dma((rows,)), dma((1,)),
            dma((2, ITERS, tiles)), dma((2, ITERS, tiles)),
            dma((2,)), dma((2,)),
            dma((ITERS, tiles, peers, 2)), dma((ITERS, tiles, peers, 2)),
        ],
        compiler_params=pltpu.CompilerParams(
            collective_id=0, has_side_effects=True, vmem_limit_bytes=50 * 1024 * 1024),
    )(x, weight_map)
    return jnp.transpose(out[:, :bands], (1, 0, 2))


def solution(mesh):
    placed = (P("band", "row", "col"), P("row", "col"))
    sizes = dict(mesh.shape)
    body = functools.partial(local, sizes["row"], sizes["col"], sizes["band"])
    return jax.shard_map(
        body, mesh=mesh, in_specs=placed, out_specs=P("band", "row", "col"), check_vma=False
    )
```

```python
import functools

import jax
import jax.numpy as jnp
from jax import lax
from jax.experimental import pallas as pl
from jax.experimental.pallas import tpu as pltpu
from jax.sharding import PartitionSpec as P

ITERS = 4
dual_step = 0.35
primal_step = 0.35
KEEP = 1.0 / (1.0 + primal_step)
GAIN = primal_step / (1.0 + primal_step)
STEP = GAIN * dual_step
LANES = 128
USEFUL = LANES - 2 * ITERS
MESH = pl.DeviceIdType.MESH


def kernel(n_row, n_col, n_band, x_ref, w_ref, out_ref,
           X, WV, N, U, W, QX, QY, HU, HD, E, ER, EL, WT, SC, CY, S, SE, R, RE, RB,
           in_sem, w_sem, ys, yr, xs, xr, zs, zr):
    bands, rows, cols = x_ref.shape
    tiles = N.shape[0]
    groups = bands // 8
    last = rows - 1
    ri = lax.axis_index("row")
    ci = lax.axis_index("col")
    bi = lax.axis_index("band")
    has_up = ri > 0
    has_down = ri < n_row - 1
    has_left = ci > 0
    has_right = ci < n_col - 1
    full = pl.ds(0, bands)

    fetches = [pltpu.make_async_copy(x_ref.at[:, r, :], X.at[r, 0:bands, LANES:LANES + cols], in_sem.at[0])
               for r in range(rows)]
    for copy in fetches:
        copy.start()
    fetch_w = pltpu.make_async_copy(w_ref, WV, w_sem.at[0])
    fetch_w.start()

    barrier = pltpu.get_barrier_semaphore()
    for cond, axis, target in ((has_up, "row", ri - 1), (has_down, "row", ri + 1),
                               (has_left, "col", ci - 1), (has_right, "col", ci + 1)):
        @pl.when(cond)
        def _():
            pl.semaphore_signal(barrier, inc=1, device_id={axis: target}, device_id_type=MESH)
    for d in range(1, n_band):
        pl.semaphore_signal(barrier, inc=1, device_id={"band": lax.rem(bi + d, n_band)}, device_id_type=MESH)
    count = (n_band - 1 + has_up.astype(jnp.int32) + has_down.astype(jnp.int32)
             + has_left.astype(jnp.int32) + has_right.astype(jnp.int32))

    def y_pair(k, j):
        span = pl.ds(0, N.shape[2]) if k == 0 else full
        src = N if k == 0 else W
        up = pltpu.make_async_remote_copy(
            src_ref=src.at[j, 0], dst_ref=HU.at[k, j, span], send_sem=ys.at[0, j], recv_sem=yr.at[0, k % 2, j],
            device_id={"row": ri - 1}, device_id_type=MESH)
        down = pltpu.make_async_remote_copy(
            src_ref=src.at[j, last], dst_ref=HD.at[k, j, span], send_sem=ys.at[1, j], recv_sem=yr.at[1, k % 2, j],
            device_id={"row": ri + 1}, device_id_type=MESH)
        return up, down

    def y_start(k, j):
        up, down = y_pair(k, j)

        @pl.when(has_up)
        def _():
            up.start()

        @pl.when(has_down)
        def _():
            down.start()

    def y_recv(k, j):
        up, down = y_pair(k, j)

        @pl.when(has_down)
        def _():
            up.wait_recv()

        @pl.when(has_up)
        def _():
            down.wait_recv()

    def y_sent(k, j):
        up, down = y_pair(k, j)

        @pl.when(has_up)
        def _():
            up.wait_send()

        @pl.when(has_down)
        def _():
            down.wait_send()

    def z_start(k, j, part):
        src, dst = ((S, R), (SE, RE))[part]
        for d in range(1, n_band):
            pltpu.make_async_remote_copy(
                src_ref=src.at[k, j], dst_ref=dst.at[k, j, d - 1],
                send_sem=zs.at[part], recv_sem=zr.at[k % 2, j, part],
                device_id={"band": lax.rem(bi + d, n_band)}, device_id_type=MESH).start()

    def z_recv(k, j, part):
        dst = (R, RE)[part].at[k, j]
        pltpu.make_async_copy(dst, dst, zr.at[k % 2, j, part]).wait()

    def z_sent(part):
        dst = (R, RE)[part]
        pltpu.make_async_copy(dst, dst, zs.at[part]).wait()

    def scale_of(weight, squares):
        return jnp.minimum(1.0, weight * lax.rsqrt(1.0 + squares * (1.0 / (GAIN * GAIN))))

    def sync(k, j):
        z_recv(k, j, 0)
        z_recv(k, j, 1)
        acc = S[k, j]
        edge = SE[k, j]
        for d in range(1, n_band):
            acc = acc + R[k, j, d - 1]
            edge = edge + RE[k, j, d - 1]
        SC[j, 0:rows] = scale_of(WT[j, 0:rows], acc)
        SC[j, last:last + 2] = scale_of(WT[j, last:last + 2], edge)

    def to_right(v):
        return pltpu.roll(v, 1, 1)

    def to_left(v):
        return pltpu.roll(v, LANES - 1, 1)

    def squares(qx, qy):
        return jnp.sum(qx * qx + qy * qy, axis=0, keepdims=True)

    def order(i):
        return lax.rem(i + 1, tiles)

    lane = lax.broadcasted_iota(jnp.int32, (8, LANES), 1)
    for j in range(tiles):
        column = ci * cols + j * USEFUL - ITERS + lane
        CY[j] = jnp.where((column >= 0) & (column < n_col * cols - 1), STEP, 0.0)
    S[:, :, last:rows, :] = jnp.zeros((ITERS, tiles, 1, LANES), jnp.float32)
    RB[...] = jnp.zeros_like(RB)

    @pl.when(jnp.logical_not(has_down))
    def _():
        HU[...] = jnp.zeros_like(HU)

    @pl.when(jnp.logical_not(has_up))
    def _():
        HD[...] = jnp.zeros_like(HD)

    @pl.when(jnp.logical_not(has_right))
    def _():
        ER[...] = jnp.zeros_like(ER)

    @pl.when(jnp.logical_not(has_left))
    def _():
        EL[...] = jnp.zeros_like(EL)

    fetch_w.wait()

    def put_weight(r, _):
        X[r, pl.ds(bands, 8), LANES:LANES + cols] = jnp.broadcast_to(WV[pl.ds(r, 1), :], (8, cols))
        return 0
    lax.fori_loop(0, rows, put_weight, 0)

    whole = X.at[:, 0:bands, LANES:LANES + cols]
    pltpu.make_async_copy(whole, whole, in_sem.at[0]).wait()

    pitch = 2 * ITERS
    spot = lax.broadcasted_iota(jnp.int32, (8, LANES), 1)

    def pack(g, _):
        span = pl.ds(pl.multiple_of(g * 8, 8), 8)
        acc = jnp.zeros((8, LANES), jnp.float32)
        for r in range(rows):
            at = r * pitch
            head = pltpu.roll(X[r, span, LANES:2 * LANES], at % LANES, 1)
            tail = pltpu.roll(X[r, span, cols:cols + LANES], (at + pitch) % LANES, 1)
            acc = jnp.where((spot >= at) & (spot < at + ITERS), head, acc)
            acc = jnp.where((spot >= at + ITERS) & (spot < at + pitch), tail, acc)
        E[span] = acc
        return 0
    lax.fori_loop(0, groups + 1, pack, 0)

    pl.semaphore_wait(barrier, count)

    e_left = pltpu.make_async_remote_copy(
        src_ref=E, dst_ref=ER, send_sem=xs.at[0], recv_sem=xr.at[0],
        device_id={"col": ci - 1}, device_id_type=MESH)
    e_right = pltpu.make_async_remote_copy(
        src_ref=E, dst_ref=EL, send_sem=xs.at[1], recv_sem=xr.at[1],
        device_id={"col": ci + 1}, device_id_type=MESH)

    @pl.when(has_left)
    def _():
        e_left.start()

    @pl.when(has_right)
    def _():
        e_right.start()

    def begin(j):
        base = j * USEFUL + LANES - ITERS
        at = base // LANES
        turn = base - at * LANES
        lo = pl.ds(pl.multiple_of(at * LANES, LANES), LANES)
        hi = pl.ds(pl.multiple_of(at * LANES + LANES, LANES), LANES)
        near = lax.broadcasted_iota(jnp.int32, (1, LANES), 1) < LANES - turn
        back = lax.rem(LANES - turn, LANES)

        def take(r):
            v = jnp.where(near, pltpu.roll(X[r, :, lo], back, 1), pltpu.roll(X[r, :, hi], back, 1))
            N[j, r] = v
            WT[j, r:r + 1] = v[bands:bands + 1]
            return v[0:bands]

        cy = CY[j, 0:1]
        old = take(0)
        end = take(last)
        y_start(0, j)
        for r in range(1, rows):
            new = take(r) if r < last else end
            qx = STEP * (new - old)
            qy = cy * (to_left(old) - old)
            QX[j, r - 1] = qx
            QY[j, r - 1] = qy
            S[0, j, r - 1:r] = squares(qx, qy)
            old = new
        z_start(0, j, 0)

    lag = min(3, tiles)

    def sweep(lo, hi, act, k):
        def span(lo, hi, k_edge):
            def one(i, _):
                act(order(i))
                if k_edge >= 0:
                    edges(k_edge, order(i + tiles - lag if k_edge < k else i - lag))
                return 0
            if lo < hi:
                lax.fori_loop(lo, hi, one, 0)
        span(lo, min(hi, lag), k - 1)
        span(max(lo, lag), hi, k)

    cx_last = jnp.where(has_down, STEP, 0.0)
    cx_above = jnp.where(has_up, STEP, 0.0)

    def edges(k, j):
        y_recv(k, j)
        field = N if k == 0 else W
        if k == 0:
            WT[j, rows:rows + 1] = HD[0, j, bands:bands + 1]
        cy = CY[j, 0:1]
        end, top = field[j, last, full], field[j, 0, full]
        below, above = HU[k, j, full], HD[k, j, full]
        for i, r, own, nxt, cx in ((0, last, end, below, cx_last), (1, rows, above, top, cx_above)):
            qx = cx * (nxt - own)
            qy = cy * (to_left(own) - own)
            if k > 0:
                sc = SC[j, r:r + 1]
                qx = sc * QX[j, r] + qx
                qy = sc * QY[j, r] + qy
            QX[j, r] = qx
            QY[j, r] = qy
            SE[k, j, i:i + 1] = squares(qx, qy)
        z_start(k, j, 1)

    inner = sum(1 for j in range(1, tiles) if j * USEFUL + LANES - ITERS <= cols)
    sweep(0, inner, begin, 0)

    @pl.when(has_right)
    def _():
        e_left.wait_recv()

    @pl.when(has_left)
    def _():
        e_right.wait_recv()

    def unpack(g, _):
        span = pl.ds(pl.multiple_of(g * 8, 8), 8)
        from_right, from_left = ER[span], EL[span]
        for r in range(rows):
            at = r * pitch
            X[r, span, cols + LANES:cols + 2 * LANES] = pltpu.roll(from_right, (LANES - at) % LANES, 1)
            X[r, span, 0:LANES] = pltpu.roll(from_left, (2 * LANES - at - pitch) % LANES, 1)
        return 0
    lax.fori_loop(0, groups + 1, unpack, 0)
    sweep(inner, tiles, begin, 0)

    def primal(j, r, px, pu, py, first):
        div = (px - pu) + (py - to_right(py))
        given = N[j, r, full]
        if first:
            return given + div, given
        u = U[j, r]
        return KEEP * u + (GAIN * given + div), u

    def step(k, j):
        first = k == 1
        sync(k - 1, j)
        y_sent(k - 1, j)

        def primal_row(r, px, pu, py):
            new, u = primal(j, r, px, pu, py, first)
            U[j, r] = new
            w = 2.0 * new - u
            W[j, r] = w
            return w

        def px_of(r):
            return SC[j, r:r + 1] * QX[j, r]

        def py_of(r):
            return SC[j, r:r + 1] * QY[j, r]

        px, py = px_of(0), py_of(0)
        w = primal_row(0, px, px_of(rows), py)
        end = primal_row(last, px_of(last), px_of(last - 1), py_of(last))
        y_start(k, j)
        cy = CY[j, 0:1]
        for r in range(1, rows):
            if r < last:
                px_new, py_new = px_of(r), py_of(r)
                w_new = primal_row(r, px_new, px, py_new)
            else:
                px_new, py_new, w_new = None, None, end
            qx = px + STEP * (w_new - w)
            qy = py + cy * (to_left(w) - w)
            QX[j, r - 1] = qx
            QY[j, r - 1] = qy
            S[k, j, r - 1:r] = squares(qx, qy)
            px, py, w = px_new, py_new, w_new
        z_start(k, j, 0)

    for k in range(1, ITERS):
        sweep(0, tiles, functools.partial(step, k), k)

    wide_lane = lax.broadcasted_iota(jnp.int32, (1, LANES), 1)

    def finish(j, wrap):
        sync(ITERS - 1, j)
        base = j * USEFUL + LANES - ITERS
        at = base // LANES - 1
        turn = base - (at + 1) * LANES
        if wrap:
            spot, keep = pl.ds(0, LANES), wide_lane >= USEFUL
        else:
            spot, keep = pl.ds(pl.multiple_of(at * LANES, LANES), LANES), wide_lane >= j * USEFUL - at * LANES
        pu = SC[j, rows:rows + 1] * QX[j, rows]
        for low in range(0, rows, 8):
            done = []
            for r in range(low, low + 8):
                sc = SC[j, r:r + 1]
                px = sc * QX[j, r]
                new, _ = primal(j, r, px, pu, sc * QY[j, r], False)
                turned = pltpu.roll(new, turn, 1)
                if wrap:
                    done.append(turned)
                else:
                    done.append(jnp.where(keep, turned, RB[r]))
                    RB[r] = turned
                pu = px
            block = jnp.swapaxes(jnp.stack(done, axis=0), 0, 1)
            if wrap:
                block = jnp.where(keep[None], out_ref[:, low:low + 8, spot], block)
            out_ref[:, low:low + 8, spot] = block

    def finish_rest(i, _):
        finish(i + 1, False)
        return 0

    sweep(0, lag, lambda j: finish(j, False), ITERS)
    lax.fori_loop(lag, tiles - 1, finish_rest, 0)
    finish(0, True)

    @pl.when(has_left)
    def _():
        e_left.wait_send()

    @pl.when(has_right)
    def _():
        e_right.wait_send()

    z_sent(0)
    z_sent(1)

    def drain(j, _):
        y_sent(ITERS - 1, j)
        return 0
    lax.fori_loop(0, tiles, drain, 0)


def local(n_row, n_col, n_band, noisy, weight_map):
    bands, rows, cols = noisy.shape
    padded = -(-bands // 8) * 8
    x = noisy
    if padded != bands:
        x = jnp.pad(x, ((0, padded - bands), (0, 0), (0, 0)))
    f32 = jnp.float32
    tiles = -(-cols // USEFUL)
    wide = cols + 2 * LANES
    extra = -(-(rows + 1) // 8) * 8
    peers = n_band - 1
    dma = pltpu.SemaphoreType.DMA
    vmem = pltpu.VMEM
    out = pl.pallas_call(
        functools.partial(kernel, n_row, n_col, n_band),
        out_shape=jax.ShapeDtypeStruct((padded, rows, cols), f32),
        in_specs=[pl.BlockSpec(memory_space=pltpu.HBM), pl.BlockSpec(memory_space=pltpu.HBM)],
        out_specs=pl.BlockSpec(memory_space=vmem),
        scratch_shapes=[
            vmem((rows, padded + 8, wide), f32),
            vmem((rows, cols), f32),
            vmem((tiles, rows, padded + 8, LANES), f32),
            vmem((tiles, rows, padded, LANES), f32),
            vmem((tiles, rows, padded, LANES), f32),
            vmem((tiles, rows + 1, padded, LANES), f32),
            vmem((tiles, rows + 1, padded, LANES), f32),
            vmem((ITERS, tiles, padded + 8, LANES), f32),
            vmem((ITERS, tiles, padded + 8, LANES), f32),
            vmem((padded + 8, LANES), f32),
            vmem((padded + 8, LANES), f32),
            vmem((padded + 8, LANES), f32),
            vmem((tiles, extra, LANES), f32),
            vmem((tiles, extra, LANES), f32),
            vmem((tiles, 8, LANES), f32),
            vmem((ITERS, tiles, rows, LANES), f32),
            vmem((ITERS, tiles, 2, LANES), f32),
            vmem((ITERS, tiles, peers, rows, LANES), f32),
            vmem((ITERS, tiles, peers, 2, LANES), f32),
            vmem((rows, padded, LANES), f32),
            dma((1,)), dma((1,)),
            dma((2, tiles)), dma((2, 2, tiles)),
            dma((2,)), dma((2,)),
            dma((2,)), dma((2, tiles, 2)),
        ],
        compiler_params=pltpu.CompilerParams(
            collective_id=0, has_side_effects=True, vmem_limit_bytes=50 * 1024 * 1024),
    )(x, weight_map)
    return out[:bands]


def solution(mesh):
    placed = (P("band", "row", "col"), P("row", "col"))
    sizes = dict(mesh.shape)
    body = functools.partial(local, sizes["row"], sizes["col"], sizes["band"])
    return jax.shard_map(
        body, mesh=mesh, in_specs=placed, out_specs=P("band", "row", "col"), check_vma=False
    )
```

```python
import functools

import jax
import jax.numpy as jnp
from jax import lax
from jax.experimental import pallas as pl
from jax.experimental.pallas import tpu as pltpu
from jax.sharding import PartitionSpec as P

ITERS = 4
dual_step = 0.35
primal_step = 0.35
KEEP = 1.0 / (1.0 + primal_step)
GAIN = primal_step / (1.0 + primal_step)
STEP = GAIN * dual_step
LANES = 128
USEFUL = LANES - 2 * ITERS
MESH = pl.DeviceIdType.MESH


def kernel(n_row, n_col, n_band, x_ref, w_ref, out_ref,
           X, WV, N, U, W, QX, QY, HU, HD, E, ER, EL, WT, SC, CY, S, SE, R, RE, RB,
           in_sem, w_sem, ys, yr, xs, xr, zs, zr):
    bands, rows, cols = x_ref.shape
    tiles = N.shape[0]
    groups = bands // 8
    last = rows - 1
    ri = lax.axis_index("row")
    ci = lax.axis_index("col")
    bi = lax.axis_index("band")
    has_up = ri > 0
    has_down = ri < n_row - 1
    has_left = ci > 0
    has_right = ci < n_col - 1
    full = pl.ds(0, bands)

    middle = max(1, cols // LANES // 2) * LANES
    parts = [(lo, hi) for lo, hi in ((0, middle), (middle, cols)) if lo < hi]

    fetch_w = pltpu.make_async_copy(w_ref, WV, w_sem.at[0])
    fetch_w.start()
    for p, (lo, hi) in enumerate(parts):
        for r in range(rows):
            pltpu.make_async_copy(x_ref.at[:, r, lo:hi], X.at[r, 0:bands, LANES + lo:LANES + hi], in_sem.at[p]).start()

    def fetched(p):
        lo, hi = parts[p]
        whole = X.at[:, 0:bands, LANES + lo:LANES + hi]
        pltpu.make_async_copy(whole, whole, in_sem.at[p]).wait()

    barrier = pltpu.get_barrier_semaphore()
    for cond, axis, target in ((has_up, "row", ri - 1), (has_down, "row", ri + 1),
                               (has_left, "col", ci - 1), (has_right, "col", ci + 1)):
        @pl.when(cond)
        def _():
            pl.semaphore_signal(barrier, inc=1, device_id={axis: target}, device_id_type=MESH)
    for d in range(1, n_band):
        pl.semaphore_signal(barrier, inc=1, device_id={"band": lax.rem(bi + d, n_band)}, device_id_type=MESH)
    count = (n_band - 1 + has_up.astype(jnp.int32) + has_down.astype(jnp.int32)
             + has_left.astype(jnp.int32) + has_right.astype(jnp.int32))

    def y_pair(k, j):
        span = pl.ds(0, N.shape[2]) if k == 0 else full
        src = N if k == 0 else W
        up = pltpu.make_async_remote_copy(
            src_ref=src.at[j, 0], dst_ref=HU.at[k, j, span], send_sem=ys.at[0, j], recv_sem=yr.at[0, k % 2, j],
            device_id={"row": ri - 1}, device_id_type=MESH)
        down = pltpu.make_async_remote_copy(
            src_ref=src.at[j, last], dst_ref=HD.at[k, j, span], send_sem=ys.at[1, j], recv_sem=yr.at[1, k % 2, j],
            device_id={"row": ri + 1}, device_id_type=MESH)
        return up, down

    def y_start(k, j):
        up, down = y_pair(k, j)

        @pl.when(has_up)
        def _():
            up.start()

        @pl.when(has_down)
        def _():
            down.start()

    def y_recv(k, j):
        up, down = y_pair(k, j)

        @pl.when(has_down)
        def _():
            up.wait_recv()

        @pl.when(has_up)
        def _():
            down.wait_recv()

    def y_sent(k, j):
        up, down = y_pair(k, j)

        @pl.when(has_up)
        def _():
            up.wait_send()

        @pl.when(has_down)
        def _():
            down.wait_send()

    def z_start(k, j, part):
        src, dst = ((S, R), (SE, RE))[part]
        for d in range(1, n_band):
            pltpu.make_async_remote_copy(
                src_ref=src.at[k, j], dst_ref=dst.at[k, j, d - 1],
                send_sem=zs.at[part], recv_sem=zr.at[k % 2, j, part],
                device_id={"band": lax.rem(bi + d, n_band)}, device_id_type=MESH).start()

    def z_recv(k, j, part):
        dst = (R, RE)[part].at[k, j]
        pltpu.make_async_copy(dst, dst, zr.at[k % 2, j, part]).wait()

    def z_sent(part):
        dst = (R, RE)[part]
        pltpu.make_async_copy(dst, dst, zs.at[part]).wait()

    def scale_of(weight, squares):
        return jnp.minimum(1.0, weight * lax.rsqrt(1.0 + squares * (1.0 / (GAIN * GAIN))))

    def sync(k, j):
        z_recv(k, j, 0)
        z_recv(k, j, 1)
        acc = S[k, j]
        edge = SE[k, j]
        for d in range(1, n_band):
            acc = acc + R[k, j, d - 1]
            edge = edge + RE[k, j, d - 1]
        SC[j, 0:rows] = scale_of(WT[j, 0:rows], acc)
        SC[j, last:last + 2] = scale_of(WT[j, last:last + 2], edge)

    def to_right(v):
        return pltpu.roll(v, 1, 1)

    def to_left(v):
        return pltpu.roll(v, LANES - 1, 1)

    def squares(qx, qy):
        return jnp.sum(qx * qx + qy * qy, axis=0, keepdims=True)

    def order(i):
        return lax.rem(i + 1, tiles)

    lane = lax.broadcasted_iota(jnp.int32, (8, LANES), 1)
    for j in range(tiles):
        column = ci * cols + j * USEFUL - ITERS + lane
        CY[j] = jnp.where((column >= 0) & (column < n_col * cols - 1), STEP, 0.0)
    S[:, :, last:rows, :] = jnp.zeros((ITERS, tiles, 1, LANES), jnp.float32)
    RB[...] = jnp.zeros_like(RB)

    @pl.when(jnp.logical_not(has_down))
    def _():
        HU[...] = jnp.zeros_like(HU)

    @pl.when(jnp.logical_not(has_up))
    def _():
        HD[...] = jnp.zeros_like(HD)

    @pl.when(jnp.logical_not(has_right))
    def _():
        ER[...] = jnp.zeros_like(ER)

    @pl.when(jnp.logical_not(has_left))
    def _():
        EL[...] = jnp.zeros_like(EL)

    fetch_w.wait()

    def put_weight(r, _):
        X[r, pl.ds(bands, 8), LANES:LANES + cols] = jnp.broadcast_to(WV[pl.ds(r, 1), :], (8, cols))
        return 0
    lax.fori_loop(0, rows, put_weight, 0)

    fetched(0)

    pitch = 2 * ITERS
    spot = lax.broadcasted_iota(jnp.int32, (8, LANES), 1)

    def pack(g, _):
        span = pl.ds(pl.multiple_of(g * 8, 8), 8)
        acc = jnp.zeros((8, LANES), jnp.float32)
        for r in range(rows):
            at = r * pitch
            head = pltpu.roll(X[r, span, LANES:2 * LANES], at % LANES, 1)
            tail = pltpu.roll(X[r, span, cols:cols + LANES], (at + pitch) % LANES, 1)
            acc = jnp.where((spot >= at) & (spot < at + ITERS), head, acc)
            acc = jnp.where((spot >= at + ITERS) & (spot < at + pitch), tail, acc)
        E[span] = acc
        return 0

    pl.semaphore_wait(barrier, count)

    e_left = pltpu.make_async_remote_copy(
        src_ref=E, dst_ref=ER, send_sem=xs.at[0], recv_sem=xr.at[0],
        device_id={"col": ci - 1}, device_id_type=MESH)
    e_right = pltpu.make_async_remote_copy(
        src_ref=E, dst_ref=EL, send_sem=xs.at[1], recv_sem=xr.at[1],
        device_id={"col": ci + 1}, device_id_type=MESH)

    def begin(j, between):
        base = j * USEFUL + LANES - ITERS
        at = base // LANES
        turn = base - at * LANES
        lo = pl.ds(pl.multiple_of(at * LANES, LANES), LANES)
        hi = pl.ds(pl.multiple_of(at * LANES + LANES, LANES), LANES)
        near = lax.broadcasted_iota(jnp.int32, (1, LANES), 1) < LANES - turn
        back = lax.rem(LANES - turn, LANES)

        def take(r):
            v = jnp.where(near, pltpu.roll(X[r, :, lo], back, 1), pltpu.roll(X[r, :, hi], back, 1))
            N[j, r] = v
            WT[j, r:r + 1] = v[bands:bands + 1]
            return v[0:bands]

        cy = CY[j, 0:1]
        old = take(0)
        end = take(last)
        y_start(0, j)
        between()
        for r in range(1, rows):
            new = take(r) if r < last else end
            qx = STEP * (new - old)
            qy = cy * (to_left(old) - old)
            QX[j, r - 1] = qx
            QY[j, r - 1] = qy
            S[0, j, r - 1:r] = squares(qx, qy)
            old = new
        z_start(0, j, 0)

    lag = min(4, tiles - 1)

    def sweep(lo, hi, act, k):
        def span(lo, hi, k_edge):
            def one(i, _):
                def middle_of():
                    if k_edge >= 0:
                        edges(k_edge, order(i + tiles - lag if k_edge < k else i - lag))
                act(order(i), middle_of)
                return 0
            if lo < hi:
                lax.fori_loop(lo, hi, one, 0)
        span(lo, min(hi, lag), k - 1)
        span(max(lo, lag), hi, k)

    cx_last = jnp.where(has_down, STEP, 0.0)
    cx_above = jnp.where(has_up, STEP, 0.0)

    def edges(k, j):
        y_recv(k, j)
        field = N if k == 0 else W
        if k == 0:
            WT[j, rows:rows + 1] = HD[0, j, bands:bands + 1]
        cy = CY[j, 0:1]
        end, top = field[j, last, full], field[j, 0, full]
        below, above = HU[k, j, full], HD[k, j, full]
        for i, r, own, nxt, cx in ((0, last, end, below, cx_last), (1, rows, above, top, cx_above)):
            qx = cx * (nxt - own)
            qy = cy * (to_left(own) - own)
            if k > 0:
                sc = SC[j, r:r + 1]
                qx = sc * QX[j, r] + qx
                qy = sc * QY[j, r] + qy
            QX[j, r] = qx
            QY[j, r] = qy
            SE[k, j, i:i + 1] = squares(qx, qy)
        z_start(k, j, 1)

    inner = sum(1 for j in range(1, tiles) if j * USEFUL + LANES - ITERS <= cols)
    early = sum(1 for j in (1, 2) if j < tiles and (j * USEFUL + LANES - ITERS) // LANES + 1 <= middle // LANES)
    sweep(0, early, begin, 0)
    for p in range(1, len(parts)):
        fetched(p)
    lax.fori_loop(0, groups + 1, pack, 0)

    @pl.when(has_left)
    def _():
        e_left.start()

    @pl.when(has_right)
    def _():
        e_right.start()

    sweep(early, inner, begin, 0)

    @pl.when(has_right)
    def _():
        e_left.wait_recv()

    @pl.when(has_left)
    def _():
        e_right.wait_recv()

    def unpack(g, _):
        span = pl.ds(pl.multiple_of(g * 8, 8), 8)
        from_right, from_left = ER[span], EL[span]
        for r in range(rows):
            at = r * pitch
            X[r, span, cols + LANES:cols + 2 * LANES] = pltpu.roll(from_right, (LANES - at) % LANES, 1)
            X[r, span, 0:LANES] = pltpu.roll(from_left, (2 * LANES - at - pitch) % LANES, 1)
        return 0
    lax.fori_loop(0, groups + 1, unpack, 0)
    sweep(inner, tiles, begin, 0)

    def primal(j, r, px, pu, py, first):
        div = (px - pu) + (py - to_right(py))
        given = N[j, r, full]
        if first:
            return given + div, given
        u = U[j, r]
        return KEEP * u + (GAIN * given + div), u

    def step(k, j, between):
        first = k == 1
        sync(k - 1, j)
        y_sent(k - 1, j)

        def primal_row(r, px, pu, py):
            new, u = primal(j, r, px, pu, py, first)
            U[j, r] = new
            w = 2.0 * new - u
            W[j, r] = w
            return w

        def px_of(r):
            return SC[j, r:r + 1] * QX[j, r]

        def py_of(r):
            return SC[j, r:r + 1] * QY[j, r]

        px, py = px_of(0), py_of(0)
        w = primal_row(0, px, px_of(rows), py)
        end = primal_row(last, px_of(last), px_of(last - 1), py_of(last))
        y_start(k, j)
        between()
        cy = CY[j, 0:1]
        for r in range(1, rows):
            if r < last:
                px_new, py_new = px_of(r), py_of(r)
                w_new = primal_row(r, px_new, px, py_new)
            else:
                px_new, py_new, w_new = None, None, end
            qx = px + STEP * (w_new - w)
            qy = py + cy * (to_left(w) - w)
            QX[j, r - 1] = qx
            QY[j, r - 1] = qy
            S[k, j, r - 1:r] = squares(qx, qy)
            px, py, w = px_new, py_new, w_new
        z_start(k, j, 0)

    for k in range(1, ITERS):
        sweep(0, tiles, functools.partial(step, k), k)

    wide_lane = lax.broadcasted_iota(jnp.int32, (1, LANES), 1)

    def finish(j, between, wrap=False):
        between()
        sync(ITERS - 1, j)
        base = j * USEFUL + LANES - ITERS
        at = base // LANES - 1
        turn = base - (at + 1) * LANES
        if wrap:
            spot, keep = pl.ds(0, LANES), wide_lane >= USEFUL
        else:
            spot, keep = pl.ds(pl.multiple_of(at * LANES, LANES), LANES), wide_lane >= j * USEFUL - at * LANES
        pu = SC[j, rows:rows + 1] * QX[j, rows]
        for low in range(0, rows, 8):
            done = []
            for r in range(low, low + 8):
                sc = SC[j, r:r + 1]
                px = sc * QX[j, r]
                py = sc * QY[j, r]
                now = KEEP * U[j, r] + (GAIN * N[j, r, full] + ((px - pu) + py))
                turned = pltpu.roll(now, turn, 1) - pltpu.roll(py, lax.rem(turn + 1, LANES), 1)
                if wrap:
                    done.append(turned)
                else:
                    done.append(jnp.where(keep, turned, RB[r]))
                    RB[r] = turned
                pu = px
            block = jnp.swapaxes(jnp.stack(done, axis=0), 0, 1)
            if wrap:
                block = jnp.where(keep[None], out_ref[:, low:low + 8, spot], block)
            out_ref[:, low:low + 8, spot] = block

    def finish_rest(i, _):
        finish(i + 1, lambda: None)
        return 0

    sweep(0, lag, finish, ITERS)
    lax.fori_loop(lag, tiles - 1, finish_rest, 0)
    finish(0, lambda: None, True)

    @pl.when(has_left)
    def _():
        e_left.wait_send()

    @pl.when(has_right)
    def _():
        e_right.wait_send()

    z_sent(0)
    z_sent(1)

    def drain(j, _):
        y_sent(ITERS - 1, j)
        return 0
    lax.fori_loop(0, tiles, drain, 0)


def local(n_row, n_col, n_band, noisy, weight_map):
    bands, rows, cols = noisy.shape
    padded = -(-bands // 8) * 8
    x = noisy
    if padded != bands:
        x = jnp.pad(x, ((0, padded - bands), (0, 0), (0, 0)))
    f32 = jnp.float32
    tiles = -(-cols // USEFUL)
    wide = cols + 2 * LANES
    extra = -(-(rows + 1) // 8) * 8
    peers = n_band - 1
    dma = pltpu.SemaphoreType.DMA
    vmem = pltpu.VMEM
    out = pl.pallas_call(
        functools.partial(kernel, n_row, n_col, n_band),
        out_shape=jax.ShapeDtypeStruct((padded, rows, cols), f32),
        in_specs=[pl.BlockSpec(memory_space=pltpu.HBM), pl.BlockSpec(memory_space=pltpu.HBM)],
        out_specs=pl.BlockSpec(memory_space=vmem),
        scratch_shapes=[
            vmem((rows, padded + 8, wide), f32),
            vmem((rows, cols), f32),
            vmem((tiles, rows, padded + 8, LANES), f32),
            vmem((tiles, rows, padded, LANES), f32),
            vmem((tiles, rows, padded, LANES), f32),
            vmem((tiles, rows + 1, padded, LANES), f32),
            vmem((tiles, rows + 1, padded, LANES), f32),
            vmem((ITERS, tiles, padded + 8, LANES), f32),
            vmem((ITERS, tiles, padded + 8, LANES), f32),
            vmem((padded + 8, LANES), f32),
            vmem((padded + 8, LANES), f32),
            vmem((padded + 8, LANES), f32),
            vmem((tiles, extra, LANES), f32),
            vmem((tiles, extra, LANES), f32),
            vmem((tiles, 8, LANES), f32),
            vmem((ITERS, tiles, rows, LANES), f32),
            vmem((ITERS, tiles, 2, LANES), f32),
            vmem((ITERS, tiles, peers, rows, LANES), f32),
            vmem((ITERS, tiles, peers, 2, LANES), f32),
            vmem((rows, padded, LANES), f32),
            dma((2,)), dma((1,)),
            dma((2, tiles)), dma((2, 2, tiles)),
            dma((2,)), dma((2,)),
            dma((2,)), dma((2, tiles, 2)),
        ],
        compiler_params=pltpu.CompilerParams(
            collective_id=0, has_side_effects=True, vmem_limit_bytes=50 * 1024 * 1024),
    )(x, weight_map)
    return out[:bands]


def solution(mesh):
    placed = (P("band", "row", "col"), P("row", "col"))
    sizes = dict(mesh.shape)
    body = functools.partial(local, sizes["row"], sizes["col"], sizes["band"])
    return jax.shard_map(
        body, mesh=mesh, in_specs=placed, out_specs=P("band", "row", "col"), check_vma=False
    )
```

```python
import functools

import jax
import jax.numpy as jnp
from jax import lax
from jax.experimental import pallas as pl
from jax.experimental.pallas import tpu as pltpu
from jax.sharding import PartitionSpec as P

ITERS = 4
dual_step = 0.35
primal_step = 0.35
KEEP = 1.0 / (1.0 + primal_step)
GAIN = primal_step / (1.0 + primal_step)
STEP = GAIN * dual_step
LANES = 128
USEFUL = LANES - 2 * ITERS
MESH = pl.DeviceIdType.MESH


def kernel(n_row, n_col, n_band, x_ref, w_ref, out_ref,
           X, WV, N, U, W, QX, QY, HU, HD, E, ER, EL, WT, SC, CY, S, SE, R, RE, RB,
           in_sem, w_sem, ys, yr, xs, xr, zs, zr):
    bands, rows, cols = x_ref.shape
    tiles = N.shape[0]
    groups = bands // 8
    last = rows - 1
    ri = lax.axis_index("row")
    ci = lax.axis_index("col")
    bi = lax.axis_index("band")
    has_up = ri > 0
    has_down = ri < n_row - 1
    has_left = ci > 0
    has_right = ci < n_col - 1
    full = pl.ds(0, bands)

    middle = max(1, cols // LANES // 2) * LANES
    parts = [(lo, hi) for lo, hi in ((0, middle), (middle, cols)) if lo < hi]

    fetch_w = pltpu.make_async_copy(w_ref, WV, w_sem.at[0])
    fetch_w.start()
    for p, (lo, hi) in enumerate(parts):
        for r in range(rows):
            pltpu.make_async_copy(x_ref.at[:, r, lo:hi], X.at[r, 0:bands, LANES + lo:LANES + hi], in_sem.at[p]).start()

    def fetched(p):
        lo, hi = parts[p]
        whole = X.at[:, 0:bands, LANES + lo:LANES + hi]
        pltpu.make_async_copy(whole, whole, in_sem.at[p]).wait()

    barrier = pltpu.get_barrier_semaphore()
    for cond, axis, target in ((has_up, "row", ri - 1), (has_down, "row", ri + 1),
                               (has_left, "col", ci - 1), (has_right, "col", ci + 1)):
        @pl.when(cond)
        def _():
            pl.semaphore_signal(barrier, inc=1, device_id={axis: target}, device_id_type=MESH)
    for d in range(1, n_band):
        pl.semaphore_signal(barrier, inc=1, device_id={"band": lax.rem(bi + d, n_band)}, device_id_type=MESH)
    count = (n_band - 1 + has_up.astype(jnp.int32) + has_down.astype(jnp.int32)
             + has_left.astype(jnp.int32) + has_right.astype(jnp.int32))

    def y_pair(k, j):
        span = pl.ds(0, N.shape[2]) if k == 0 else full
        src = N if k == 0 else W
        up = pltpu.make_async_remote_copy(
            src_ref=src.at[j, 0], dst_ref=HU.at[k, j, span], send_sem=ys.at[0, j], recv_sem=yr.at[0, k % 2, j],
            device_id={"row": ri - 1}, device_id_type=MESH)
        down = pltpu.make_async_remote_copy(
            src_ref=src.at[j, last], dst_ref=HD.at[k, j, span], send_sem=ys.at[1, j], recv_sem=yr.at[1, k % 2, j],
            device_id={"row": ri + 1}, device_id_type=MESH)
        return up, down

    def y_start(k, j):
        up, down = y_pair(k, j)

        @pl.when(has_up)
        def _():
            up.start()

        @pl.when(has_down)
        def _():
            down.start()

    def y_recv(k, j):
        up, down = y_pair(k, j)

        @pl.when(has_down)
        def _():
            up.wait_recv()

        @pl.when(has_up)
        def _():
            down.wait_recv()

    def y_sent(k, j):
        up, down = y_pair(k, j)

        @pl.when(has_up)
        def _():
            up.wait_send()

        @pl.when(has_down)
        def _():
            down.wait_send()

    def z_start(k, j, part):
        src, dst = ((S, R), (SE, RE))[part]
        span = pl.ds(0, (last, 2)[part])
        for d in range(1, n_band):
            pltpu.make_async_remote_copy(
                src_ref=src.at[k, j, span], dst_ref=dst.at[k, j, d - 1, span],
                send_sem=zs.at[part], recv_sem=zr.at[k % 2, j, part],
                device_id={"band": lax.rem(bi + d, n_band)}, device_id_type=MESH).start()

    def z_recv(k, j, part):
        dst = (R, RE)[part].at[k, j, :, pl.ds(0, (last, 2)[part])]
        pltpu.make_async_copy(dst, dst, zr.at[k % 2, j, part]).wait()

    def z_sent(part):
        dst = (R, RE)[part].at[:, :, :, pl.ds(0, (last, 2)[part])]
        pltpu.make_async_copy(dst, dst, zs.at[part]).wait()

    def scale_of(weight, squares):
        return jnp.minimum(1.0, weight * lax.rsqrt(1.0 + squares * (1.0 / (GAIN * GAIN))))

    def sync(k, j):
        z_recv(k, j, 0)
        z_recv(k, j, 1)
        acc = S[k, j, 0:last]
        edge = SE[k, j]
        for d in range(1, n_band):
            acc = acc + R[k, j, d - 1, 0:last]
            edge = edge + RE[k, j, d - 1]
        SC[j, 0:last] = scale_of(WT[j, 0:last], acc)
        SC[j, last:last + 2] = scale_of(WT[j, last:last + 2], edge)

    def to_right(v):
        return pltpu.roll(v, 1, 1)

    def to_left(v):
        return pltpu.roll(v, LANES - 1, 1)

    def squares(qx, qy):
        return jnp.sum(qx * qx + qy * qy, axis=0, keepdims=True)

    def order(i):
        return lax.rem(i + 1, tiles)

    lane = lax.broadcasted_iota(jnp.int32, (8, LANES), 1)
    for j in range(tiles):
        column = ci * cols + j * USEFUL - ITERS + lane
        CY[j] = jnp.where((column >= 0) & (column < n_col * cols - 1), STEP, 0.0)
    RB[...] = jnp.zeros_like(RB)

    @pl.when(jnp.logical_not(has_down))
    def _():
        HU[...] = jnp.zeros_like(HU)

    @pl.when(jnp.logical_not(has_up))
    def _():
        HD[...] = jnp.zeros_like(HD)

    @pl.when(jnp.logical_not(has_right))
    def _():
        ER[...] = jnp.zeros_like(ER)

    @pl.when(jnp.logical_not(has_left))
    def _():
        EL[...] = jnp.zeros_like(EL)

    fetch_w.wait()

    def put_weight(r, _):
        X[r, pl.ds(bands, 8), LANES:LANES + cols] = jnp.broadcast_to(WV[pl.ds(r, 1), :], (8, cols))
        return 0
    lax.fori_loop(0, rows, put_weight, 0)

    fetched(0)

    pitch = 2 * ITERS
    spot = lax.broadcasted_iota(jnp.int32, (8, LANES), 1)

    def pack(g, _):
        span = pl.ds(pl.multiple_of(g * 8, 8), 8)
        acc = jnp.zeros((8, LANES), jnp.float32)
        for r in range(rows):
            at = r * pitch
            head = pltpu.roll(X[r, span, LANES:2 * LANES], at % LANES, 1)
            tail = pltpu.roll(X[r, span, cols:cols + LANES], (at + pitch) % LANES, 1)
            acc = jnp.where((spot >= at) & (spot < at + ITERS), head, acc)
            acc = jnp.where((spot >= at + ITERS) & (spot < at + pitch), tail, acc)
        E[span] = acc
        return 0

    pl.semaphore_wait(barrier, count)

    e_left = pltpu.make_async_remote_copy(
        src_ref=E, dst_ref=ER, send_sem=xs.at[0], recv_sem=xr.at[0],
        device_id={"col": ci - 1}, device_id_type=MESH)
    e_right = pltpu.make_async_remote_copy(
        src_ref=E, dst_ref=EL, send_sem=xs.at[1], recv_sem=xr.at[1],
        device_id={"col": ci + 1}, device_id_type=MESH)

    def begin(j, between):
        base = j * USEFUL + LANES - ITERS
        at = base // LANES
        turn = base - at * LANES
        lo = pl.ds(pl.multiple_of(at * LANES, LANES), LANES)
        hi = pl.ds(pl.multiple_of(at * LANES + LANES, LANES), LANES)
        near = lax.broadcasted_iota(jnp.int32, (1, LANES), 1) < LANES - turn
        back = lax.rem(LANES - turn, LANES)

        def take(r):
            v = jnp.where(near, pltpu.roll(X[r, :, lo], back, 1), pltpu.roll(X[r, :, hi], back, 1))
            N[j, r] = v
            WT[j, r:r + 1] = v[bands:bands + 1]
            return v[0:bands]

        cy = CY[j, 0:1]
        old = take(0)
        end = take(last)
        y_start(0, j)
        between()
        for r in range(1, rows):
            new = take(r) if r < last else end
            qx = STEP * (new - old)
            qy = cy * (to_left(old) - old)
            QX[j, r - 1] = qx
            QY[j, r - 1] = qy
            S[0, j, r - 1:r] = squares(qx, qy)
            old = new
        z_start(0, j, 0)

    lag = min(4, tiles - 1)

    def sweep(lo, hi, act, k):
        def span(lo, hi, k_edge):
            def one(i, _):
                def middle_of():
                    if k_edge >= 0:
                        edges(k_edge, order(i + tiles - lag if k_edge < k else i - lag))
                act(order(i), middle_of)
                return 0
            if lo < hi:
                lax.fori_loop(lo, hi, one, 0)
        span(lo, min(hi, lag), k - 1)
        span(max(lo, lag), hi, k)

    cx_last = jnp.where(has_down, STEP, 0.0)
    cx_above = jnp.where(has_up, STEP, 0.0)

    def edges(k, j):
        y_recv(k, j)
        field = N if k == 0 else W
        if k == 0:
            WT[j, rows:rows + 1] = HD[0, j, bands:bands + 1]
        cy = CY[j, 0:1]
        end, top = field[j, last, full], field[j, 0, full]
        below, above = HU[k, j, full], HD[k, j, full]
        for i, r, own, nxt, cx in ((0, last, end, below, cx_last), (1, rows, above, top, cx_above)):
            qx = cx * (nxt - own)
            qy = cy * (to_left(own) - own)
            if k > 0:
                sc = SC[j, r:r + 1]
                qx = sc * QX[j, r] + qx
                qy = sc * QY[j, r] + qy
            QX[j, r] = qx
            QY[j, r] = qy
            SE[k, j, i:i + 1] = squares(qx, qy)
        z_start(k, j, 1)

    inner = sum(1 for j in range(1, tiles) if j * USEFUL + LANES - ITERS <= cols)
    early = sum(1 for j in (1, 2) if j < tiles and (j * USEFUL + LANES - ITERS) // LANES + 1 <= middle // LANES)
    sweep(0, early, begin, 0)
    for p in range(1, len(parts)):
        fetched(p)
    lax.fori_loop(0, groups + 1, pack, 0)

    @pl.when(has_left)
    def _():
        e_left.start()

    @pl.when(has_right)
    def _():
        e_right.start()

    sweep(early, inner, begin, 0)

    @pl.when(has_right)
    def _():
        e_left.wait_recv()

    @pl.when(has_left)
    def _():
        e_right.wait_recv()

    def unpack(g, _):
        span = pl.ds(pl.multiple_of(g * 8, 8), 8)
        from_right, from_left = ER[span], EL[span]
        for r in range(rows):
            at = r * pitch
            X[r, span, cols + LANES:cols + 2 * LANES] = pltpu.roll(from_right, (LANES - at) % LANES, 1)
            X[r, span, 0:LANES] = pltpu.roll(from_left, (2 * LANES - at - pitch) % LANES, 1)
        return 0
    lax.fori_loop(0, groups + 1, unpack, 0)
    sweep(inner, tiles, begin, 0)

    def primal(j, r, px, pu, py, first):
        div = (px - pu) + (py - to_right(py))
        given = N[j, r, full]
        if first:
            return given + div, given
        u = U[j, r]
        return KEEP * u + (GAIN * given + div), u

    def step(k, j, between):
        first = k == 1
        sync(k - 1, j)
        y_sent(k - 1, j)

        def primal_row(r, px, pu, py):
            new, u = primal(j, r, px, pu, py, first)
            U[j, r] = new
            w = 2.0 * new - u
            W[j, r] = w
            return w

        def px_of(r):
            return SC[j, r:r + 1] * QX[j, r]

        def py_of(r):
            return SC[j, r:r + 1] * QY[j, r]

        primal_row(0, px_of(0), px_of(rows), py_of(0))
        primal_row(last, px_of(last), px_of(last - 1), py_of(last))
        y_start(k, j)
        between()
        cy = CY[j, 0:1]
        total = [0.0] * last
        for g in range(groups):
            span = pl.ds(g * 8, 8)
            px = SC[j, 0:1] * QX[j, 0, span]
            py = SC[j, 0:1] * QY[j, 0, span]
            w = W[j, 0, span]
            for r in range(1, rows):
                if r < last:
                    sc = SC[j, r:r + 1]
                    px_new = sc * QX[j, r, span]
                    py_new = sc * QY[j, r, span]
                    div = (px_new - px) + (py_new - to_right(py_new))
                    given = N[j, r, span]
                    if first:
                        u, new = given, given + div
                    else:
                        u = U[j, r, span]
                        new = KEEP * u + (GAIN * given + div)
                    U[j, r, span] = new
                    w_new = 2.0 * new - u
                else:
                    px_new, py_new, w_new = None, None, W[j, last, span]
                qx = px + STEP * (w_new - w)
                qy = py + cy * (to_left(w) - w)
                QX[j, r - 1, span] = qx
                QY[j, r - 1, span] = qy
                total[r - 1] = total[r - 1] + (qx * qx + qy * qy)
                px, py, w = px_new, py_new, w_new
        for r in range(1, rows):
            S[k, j, r - 1:r] = jnp.sum(total[r - 1], axis=0, keepdims=True)
        z_start(k, j, 0)

    for k in range(1, ITERS):
        sweep(0, tiles, functools.partial(step, k), k)

    wide_lane = lax.broadcasted_iota(jnp.int32, (1, LANES), 1)

    def finish(j, between, wrap=False):
        between()
        sync(ITERS - 1, j)
        base = j * USEFUL + LANES - ITERS
        at = base // LANES - 1
        turn = base - (at + 1) * LANES
        if wrap:
            spot, keep = pl.ds(0, LANES), wide_lane >= USEFUL
        else:
            spot, keep = pl.ds(pl.multiple_of(at * LANES, LANES), LANES), wide_lane >= j * USEFUL - at * LANES
        pu = SC[j, rows:rows + 1] * QX[j, rows]
        for low in range(0, rows, 8):
            done = []
            for r in range(low, low + 8):
                sc = SC[j, r:r + 1]
                px = sc * QX[j, r]
                py = sc * QY[j, r]
                now = KEEP * U[j, r] + (GAIN * N[j, r, full] + ((px - pu) + py))
                turned = pltpu.roll(now, turn, 1) - pltpu.roll(py, lax.rem(turn + 1, LANES), 1)
                if wrap:
                    done.append(turned)
                else:
                    done.append(jnp.where(keep, turned, RB[r]))
                    RB[r] = turned
                pu = px
            block = jnp.swapaxes(jnp.stack(done, axis=0), 0, 1)
            if wrap:
                block = jnp.where(keep[None], out_ref[:, low:low + 8, spot], block)
            out_ref[:, low:low + 8, spot] = block

    def finish_rest(i, _):
        finish(i + 1, lambda: None)
        return 0

    sweep(0, lag, finish, ITERS)
    lax.fori_loop(lag, tiles - 1, finish_rest, 0)
    finish(0, lambda: None, True)

    @pl.when(has_left)
    def _():
        e_left.wait_send()

    @pl.when(has_right)
    def _():
        e_right.wait_send()

    z_sent(0)
    z_sent(1)

    def drain(j, _):
        y_sent(ITERS - 1, j)
        return 0
    lax.fori_loop(0, tiles, drain, 0)


def local(n_row, n_col, n_band, noisy, weight_map):
    bands, rows, cols = noisy.shape
    padded = -(-bands // 8) * 8
    x = noisy
    if padded != bands:
        x = jnp.pad(x, ((0, padded - bands), (0, 0), (0, 0)))
    f32 = jnp.float32
    tiles = -(-cols // USEFUL)
    wide = cols + 2 * LANES
    extra = -(-(rows + 1) // 8) * 8
    peers = n_band - 1
    dma = pltpu.SemaphoreType.DMA
    vmem = pltpu.VMEM
    out = pl.pallas_call(
        functools.partial(kernel, n_row, n_col, n_band),
        out_shape=jax.ShapeDtypeStruct((padded, rows, cols), f32),
        in_specs=[pl.BlockSpec(memory_space=pltpu.HBM), pl.BlockSpec(memory_space=pltpu.HBM)],
        out_specs=pl.BlockSpec(memory_space=vmem),
        scratch_shapes=[
            vmem((rows, padded + 8, wide), f32),
            vmem((rows, cols), f32),
            vmem((tiles, rows, padded + 8, LANES), f32),
            vmem((tiles, rows, padded, LANES), f32),
            vmem((tiles, rows, padded, LANES), f32),
            vmem((tiles, rows + 1, padded, LANES), f32),
            vmem((tiles, rows + 1, padded, LANES), f32),
            vmem((ITERS, tiles, padded + 8, LANES), f32),
            vmem((ITERS, tiles, padded + 8, LANES), f32),
            vmem((padded + 8, LANES), f32),
            vmem((padded + 8, LANES), f32),
            vmem((padded + 8, LANES), f32),
            vmem((tiles, extra, LANES), f32),
            vmem((tiles, extra, LANES), f32),
            vmem((tiles, 8, LANES), f32),
            vmem((ITERS, tiles, rows, LANES), f32),
            vmem((ITERS, tiles, 2, LANES), f32),
            vmem((ITERS, tiles, peers, rows, LANES), f32),
            vmem((ITERS, tiles, peers, 2, LANES), f32),
            vmem((rows, padded, LANES), f32),
            dma((2,)), dma((1,)),
            dma((2, tiles)), dma((2, 2, tiles)),
            dma((2,)), dma((2,)),
            dma((2,)), dma((2, tiles, 2)),
        ],
        compiler_params=pltpu.CompilerParams(
            collective_id=0, has_side_effects=True, vmem_limit_bytes=50 * 1024 * 1024),
    )(x, weight_map)
    return out[:bands]


def solution(mesh):
    placed = (P("band", "row", "col"), P("row", "col"))
    sizes = dict(mesh.shape)
    body = functools.partial(local, sizes["row"], sizes["col"], sizes["band"])
    return jax.shard_map(
        body, mesh=mesh, in_specs=placed, out_specs=P("band", "row", "col"), check_vma=False
    )
```
